32 devices in a mesh: dp: 4 (over y, x), tensor: 8 (over z, core).
Axes of the slice: x: 2, y: 2, z: 4, core: 2. Of those that a mesh axis runs over, the one named last changes fastest.
Arguments:
- new_weight: float32 [5376, 8192], P(('dp', 'tensor')), may hold values from -0.0625 to 0.0625
- synced_weight: float32 [5376, 8192], P(('dp', 'tensor')), may hold values from -0.0625 to 0.0625
- resident: bfloat16 [5376, 8192], P(None, 'tensor'), may hold values from -0.0625 to 0.0625
- gain: float32 [5376], replicated, may hold values from 0.5 to 1.5
- query: bfloat16 [32, 2, 8192], P(('dp', 'tensor')), may hold values from -256 to 256
- cache_keys: bfloat16 [32, 768, 1024], P(('dp', 'tensor')), may hold values from -8 to 8
- cache_values: bfloat16 [32, 768, 1024], P(('dp', 'tensor')), may hold values from -6 to 6
- new_keys: bfloat16 [32, 2, 1024], P(('dp', 'tensor')), may hold values from -6 to 6
- new_values: bfloat16 [32, 2, 1024], P(('dp', 'tensor')), may hold values from -6 to 6
- cache_lengths: int32 [32], P(('dp', 'tensor')), may hold values from 2 to 768, as said below
Outputs:
- normed: bfloat16 [32, 2, 5376], P(('dp', 'tensor'))
The draws below stay inside these ranges and needn't reach their ends.
Inputs may be any that keep to these rules, and one draw needn't show every extreme that they name: `cache_lengths`: some row has all 768 slots filled.
All inputs are finite; a program needn't handle non-finite values.
Results may differ from the reference program's by a relative error of at most 0.0069.
Values may be sent and summed in bfloat16 or wider, within the bound.
No kernel may reach another device: no remote copies, remote signals or barrier semaphores. Data moves between devices by JAX's collectives and lax.ppermute only.
A program may use at most 128 MiB of HBM per device.

```python
import jax
import jax.numpy as jnp
from jax import lax

HEADS = 64
KVH = 8
HD = 128
D = 8192
DW = 5376
NEW = 2
CTX = 768
ROWS = 32


def draw_query(key, part):
    sample = jax.random.normal(jax.random.fold_in(key, 3), (ROWS, NEW, HEADS, HD), jnp.float32)
    sample = jnp.clip(sample, -6.0, 6.0)
    return sample.reshape(ROWS, NEW, HEADS * HD).astype(jnp.bfloat16)


def draw_cache_keys(key, part):
    sample = jax.random.normal(jax.random.fold_in(key, 9), (ROWS, CTX, KVH, HD), jnp.float32)
    sample = jnp.clip(sample, -6.0, 6.0)
    return sample.reshape(ROWS, CTX, KVH * HD).astype(jnp.bfloat16)


def draw_cache_lengths(key, part):
    drawn = jax.random.randint(jax.random.fold_in(key, 13), (ROWS,), 2, CTX + 1)
    return drawn.at[0].set(CTX).astype(jnp.int32)


def level_of(key, extent, split, least, high):
    def one(axis_at, parts):
        steps = jax.random.uniform(jax.random.fold_in(jax.random.fold_in(key, 6), axis_at), (parts,), jnp.float32, least / len(split), high / len(split))
        return jnp.repeat(jnp.exp(steps), extent[axis_at] // parts).reshape((-1,) + (1,) * (len(extent) - axis_at - 1))

    loudness = one(*split[0])
    for cut in split[1:]:
        loudness = loudness * one(*cut)
    return loudness


def gaussian(rng, dims, spread, most, split=(), held_as=jnp.bfloat16):
    values = spread * jax.random.normal(rng, dims, jnp.float32)
    if split:
        values = values * level_of(rng, dims, split, -0.22, 0.18)
    return jnp.clip(values, -most, most).astype(held_as)


def setup_inputs(seed: int = 0) -> dict:
    arg_keys = jax.random.split(jax.random.key(seed), 11)
    new_weight = gaussian(arg_keys[0], (DW, D), D ** -0.5, 0.0625, ((0, 32),), jnp.float32)
    synced_weight = gaussian(arg_keys[1], (DW, D), D ** -0.5, 0.0625, ((0, 32),), jnp.float32)
    resident = gaussian(arg_keys[2], (DW, D), D ** -0.5, 0.0625, ((1, 8),))
    gain = jnp.clip(1.0 + 0.1 * jax.random.normal(arg_keys[3], (DW,), jnp.float32), 0.5, 1.5)
    query = draw_query(jax.random.fold_in(arg_keys[10], 71), 0)
    cache_keys = draw_cache_keys(jax.random.fold_in(arg_keys[10], 71), 0)
    cache_values = gaussian(arg_keys[6], (ROWS, CTX, KVH * HD), 1.0, 6.0, ((0, 32),))
    new_keys = gaussian(arg_keys[7], (ROWS, NEW, KVH * HD), 1.0, 6.0, ((0, 32),))
    new_values = gaussian(arg_keys[8], (ROWS, NEW, KVH * HD), 1.0, 6.0, ((0, 32),))
    cache_lengths = draw_cache_lengths(jax.random.fold_in(arg_keys[10], 71), 0)
    return {"new_weight": new_weight, "synced_weight": synced_weight, "resident": resident, "gain": gain, "query": query, "cache_keys": cache_keys, "cache_values": cache_values, "new_keys": new_keys, "new_values": new_values, "cache_lengths": cache_lengths}


def attend_row(packed):
    queries, keys_old, values_old, keys_new, values_new, valid_length = packed
    grouping = HEADS // KVH
    factor = HD ** (-0.5)
    queries = queries.astype(jnp.float32).reshape(NEW, KVH, grouping, HD)
    keys_old = keys_old.astype(jnp.float32).reshape(CTX, KVH, HD)
    values_old = values_old.astype(jnp.float32).reshape(CTX, KVH, HD)
    keys_new = keys_new.astype(jnp.float32).reshape(NEW, KVH, HD)
    values_new = values_new.astype(jnp.float32).reshape(NEW, KVH, HD)
    past_scores = jnp.einsum('jkgd,pkd->jkgp', queries, keys_old) * factor
    own_scores = jnp.einsum('jkgd,ikd->jkgi', queries, keys_new) * factor
    past_valid = (jnp.arange(CTX).astype(jnp.int32) < valid_length)[None, None, None, :]
    positions = jnp.arange(NEW).astype(jnp.int32)
    own_valid = (positions[None, :] <= positions[:, None])[:, None, None, :]
    past_scores = jnp.where(past_valid, past_scores, -jnp.inf)
    own_scores = jnp.where(own_valid, own_scores, -jnp.inf)
    highest = jnp.maximum(lax.optimization_barrier(jnp.max(past_scores, axis=-1, keepdims=True)), lax.optimization_barrier(jnp.max(own_scores, axis=-1, keepdims=True)))
    past_exp = jnp.exp(past_scores - highest)
    own_exp = jnp.exp(own_scores - highest)
    total = lax.optimization_barrier(jnp.sum(past_exp, axis=-1, keepdims=True)) + lax.optimization_barrier(jnp.sum(own_exp, axis=-1, keepdims=True))
    past_probs = lax.optimization_barrier((past_exp / total).astype(jnp.bfloat16)).astype(jnp.float32)
    own_probs = lax.optimization_barrier((own_exp / total).astype(jnp.bfloat16)).astype(jnp.float32)
    attended = jnp.einsum('jkgp,pkd->jkgd', past_probs, values_old) + jnp.einsum('jkgi,ikd->jkgd', own_probs, values_new)
    return attended.reshape(NEW, HEADS * HD).astype(jnp.bfloat16)

def reference(new_weight, synced_weight, resident, gain, query, cache_keys, cache_values, new_keys, new_values, cache_lengths):
    change = (new_weight - synced_weight).astype(jnp.bfloat16)
    weight = (resident.astype(jnp.float32) + change.astype(jnp.float32)).astype(jnp.bfloat16)
    attended = lax.map(attend_row, (query, cache_keys, cache_values, new_keys, new_values, cache_lengths))
    flat_rows = attended.reshape(ROWS * NEW, HEADS * HD)
    projected = jnp.dot(flat_rows, weight.T, preferred_element_type=jnp.float32)
    mean_square = lax.optimization_barrier(jnp.mean(projected * projected, axis=-1, keepdims=True))
    normed = projected * lax.rsqrt(mean_square + 1e-06) * gain
    return normed.reshape(ROWS, NEW, DW).astype(jnp.bfloat16)
```

```python
import functools

import jax
import jax.numpy as jnp
from jax import lax
from jax.experimental import pallas as pl
from jax.experimental.pallas import tpu as pltpu
from jax.sharding import PartitionSpec as P

HD = 128
CORES = 2
MOST = 32
FEW = 4
NT = (((1,), (1,)), ((), ()))
NN = (((1,), (0,)), ((), ()))


def dot(a, b, dims):
    return lax.dot_general(a, b, dims, preferred_element_type=jnp.float32)


def divisor(total, most, unit):
    fits = [n for n in range(unit, min(total, most) + 1, unit) if total % n == 0]
    return fits[-1] if fits else total


def attend_kernel(length_ref, query_ref, keys_ref, values_ref, new_keys_ref, new_values_ref, out_ref, *, grouping):
    steps, width = new_keys_ref.shape[1], new_keys_ref.shape[2]
    heads = width // HD
    slots = keys_ref.shape[1]
    factor = HD ** (-0.5)
    query = query_ref[0].astype(jnp.float32)
    block_rows = grouping * steps
    rows = heads * block_rows
    bands = []
    for k in range(heads):
        pieces = [query[:, (k * grouping + g) * HD : (k * grouping + g + 1) * HD] for g in range(grouping)]
        own = jnp.concatenate(pieces, axis=0)
        line = [own if i == k else jnp.zeros_like(own) for i in range(heads)]
        bands.append(jnp.concatenate(line, axis=1))
    stacked = jnp.concatenate(bands, axis=0).astype(jnp.bfloat16)

    padding = jnp.zeros((8 - steps % 8, width), jnp.float32)
    keys_new = jnp.concatenate([new_keys_ref[0].astype(jnp.float32), padding], axis=0).astype(jnp.bfloat16)
    values_new = jnp.concatenate([new_values_ref[0].astype(jnp.float32), padding], axis=0).astype(jnp.bfloat16)

    past = dot(stacked, keys_ref[0], NT) * factor
    own = dot(stacked, keys_new, NT) * factor
    slot = lax.broadcasted_iota(jnp.int32, past.shape, 1)
    past = jnp.where(slot < length_ref[pl.program_id(0)], past, -jnp.inf)
    column = lax.broadcasted_iota(jnp.int32, own.shape, 1)
    position = lax.rem(lax.broadcasted_iota(jnp.int32, own.shape, 0), steps)
    own = jnp.where(column <= position, own, -jnp.inf)
    highest = jnp.maximum(jnp.max(past, axis=1, keepdims=True), jnp.max(own, axis=1, keepdims=True))
    past = jnp.exp(past - highest)
    own = jnp.exp(own - highest)
    total = jnp.sum(past, axis=1, keepdims=True) + jnp.sum(own, axis=1, keepdims=True)
    past = (past / total).astype(jnp.bfloat16)
    own = (own / total).astype(jnp.bfloat16)
    attended = dot(past, values_ref[0], NN) + dot(own, values_new, NN)
    for k in range(heads):
        for g in range(grouping):
            at = k * block_rows + g * steps
            head = k * grouping + g
            out_ref[0, :, head * HD : (head + 1) * HD] = attended[at : at + steps, k * HD : (k + 1) * HD].astype(
                jnp.bfloat16
            )


def attend(query, cache_keys, cache_values, new_keys, new_values, cache_lengths):
    rows, steps, features = query.shape
    slots, kv_features = cache_keys.shape[1:]
    grouping = features // kv_features
    width = HD * 2 if kv_features % (HD * 2) == 0 else HD
    wide = lambda r, h, *_: (r, 0, h)
    return pl.pallas_call(
        functools.partial(attend_kernel, grouping=grouping),
        out_shape=jax.ShapeDtypeStruct(query.shape, jnp.bfloat16),
        grid_spec=pltpu.PrefetchScalarGridSpec(
            num_scalar_prefetch=1,
            grid=(rows, kv_features // width),
            in_specs=[
                pl.BlockSpec((1, steps, width * grouping), wide),
                pl.BlockSpec((1, slots, width), wide),
                pl.BlockSpec((1, slots, width), wide),
                pl.BlockSpec((1, steps, width), wide),
                pl.BlockSpec((1, steps, width), wide),
            ],
            out_specs=pl.BlockSpec((1, steps, width * grouping), wide),
        ),
        name="attend",
    )(cache_lengths, query, cache_keys, cache_values, new_keys, new_values)


def weights_kernel(group_ref, new_ref, synced_ref, resident_ref, out_ref):
    blocks, depth = out_ref.shape[1], out_ref.shape[3]
    for b in range(blocks):
        at = slice(b * depth, (b + 1) * depth)
        out_ref[0, b] = (new_ref[:, at] - synced_ref[:, at]).astype(jnp.bfloat16)
    out_ref[1] = resident_ref[...]


def local_weights(new_weight, synced_weight, resident, group, groups):
    rows, features = new_weight.shape
    depth = resident.shape[1]
    blocks = features // depth
    stored = resident.reshape(groups * blocks, rows, depth)
    take = divisor(rows, 24, 8)
    return pl.pallas_call(
        weights_kernel,
        out_shape=jax.ShapeDtypeStruct((2, blocks, rows, depth), jnp.bfloat16),
        grid_spec=pltpu.PrefetchScalarGridSpec(
            num_scalar_prefetch=1,
            grid=(rows // take,),
            in_specs=[
                pl.BlockSpec((take, features), lambda i, g: (i, 0)),
                pl.BlockSpec((take, features), lambda i, g: (i, 0)),
                pl.BlockSpec((blocks, take, depth), lambda i, g: (g[0], i, 0)),
            ],
            out_specs=pl.BlockSpec((2, blocks, take, depth), lambda i, g: (0, 0, i, 0)),
        ),
        name="local_weights",
    )(group, new_weight, synced_weight, stored)


def project_kernel(place_ref, *refs, parts):
    gathered, (own_ref, other_ref, out_ref, rows_ref, sums_ref) = refs[:parts], refs[parts:]
    owners, steps, columns = out_ref.shape
    blocks, width, depth = own_ref.shape[1:]
    first = pl.program_id(0) * owners
    pieces = []
    for part in gathered:
        for k in range(part.shape[0]):
            pieces.append(part[k].astype(jnp.float32))
    rows_ref[...] = jnp.concatenate(pieces, axis=0).astype(jnp.bfloat16)
    for source, ref in enumerate((own_ref, other_ref)):
        block = place_ref[source]
        rows = rows_ref[:, pl.ds(pl.multiple_of(block * depth, depth), depth)]
        for b in range(blocks):
            value = dot(rows, ref[1, b], NT)
            if source == 0:
                sums_ref[b] = value
            else:
                sums_ref[b] += value
    for source, ref in enumerate((own_ref, other_ref)):
        value = dot(rows_ref[:, :depth], ref[0, 0], NT)
        for b in range(1, blocks):
            value += dot(rows_ref[:, b * depth : (b + 1) * depth], ref[0, b], NT)
        sums_ref[place_ref[source]] += value
    for k in range(owners):
        owner = place_ref[2 + first + k] - first
        at = slice(k * steps, (k + 1) * steps)
        for b in range(blocks):
            out_ref[owner, :, b * width : (b + 1) * width] = sums_ref[b, at, :]


def project(gathered, own, other, place, owners, steps):
    blocks, width, depth = own.shape[1:]
    take = owners if len(gathered) > 1 else divisor(owners, MOST, 1)
    several = owners > take
    whole = pl.BlockSpec(memory_space=pltpu.VMEM)
    cut = lambda s: pl.BlockSpec((take, *s[1:]), lambda i: (i, 0, 0)) if several else whole
    out = jax.ShapeDtypeStruct((owners, steps, blocks * width), jnp.float32)
    return pl.pallas_call(
        functools.partial(project_kernel, parts=len(gathered)),
        out_shape=out,
        grid=(owners // take,),
        in_specs=[pl.BlockSpec(memory_space=pltpu.SMEM), *[cut(g.shape) for g in gathered], whole, whole],
        out_specs=cut(out.shape),
        scratch_shapes=[
            pltpu.VMEM((take * steps, blocks * depth), jnp.bfloat16),
            pltpu.VMEM((blocks, take * steps, width), jnp.float32),
        ],
        name="project",
    )(place, *gathered, own, other)


def norm_kernel(partial_ref, gain_ref, out_ref, sums_ref, *, groups):
    owners, steps, columns = partial_ref.shape
    chips = owners // groups
    for d in range(groups):
        value = partial_ref[d * chips]
        for z in range(1, chips):
            value += partial_ref[d * chips + z]
        sums_ref[:, d * columns : (d + 1) * columns] = value
    projected = sums_ref[...]
    mean_square = jnp.mean(projected * projected, axis=1, keepdims=True)
    out_ref[0] = (projected * lax.rsqrt(mean_square + 1e-06) * gain_ref[...]).astype(jnp.bfloat16)


def normalise(partial, gain, groups):
    steps, columns = partial.shape[1], partial.shape[2] * groups
    return pl.pallas_call(
        functools.partial(norm_kernel, groups=groups),
        out_shape=jax.ShapeDtypeStruct((1, steps, columns), jnp.bfloat16),
        in_specs=[pl.BlockSpec(memory_space=pltpu.VMEM)] * 2,
        out_specs=pl.BlockSpec(memory_space=pltpu.VMEM),
        scratch_shapes=[pltpu.VMEM((steps, columns), jnp.float32)],
        name="normalise",
    )(partial, gain.reshape(1, columns))


def body(
    new_weight,
    synced_weight,
    resident,
    gain,
    query,
    cache_keys,
    cache_values,
    new_keys,
    new_values,
    cache_lengths,
):
    groups, devices = lax.axis_size("dp"), lax.axis_size("tensor")
    chips = devices // CORES
    group, device = lax.axis_index("dp"), lax.axis_index("tensor")
    chip = device // CORES
    count, steps, features = query.shape

    def exchange(value, axis, size, unit, hop):
        return lax.ppermute(value, axis, [(i, (i // unit ^ hop) * unit + i % unit) for i in range(size)])

    attended = attend(query, cache_keys, cache_values, new_keys, new_values, cache_lengths)
    if chips <= FEW and chips & (chips - 1) == 0:
        column = jnp.concatenate(
            [attended] + [exchange(attended, "tensor", devices, CORES, hop) for hop in range(1, chips)], axis=0
        )
        chip_order = [chip ^ hop for hop in range(chips)]
    else:
        alike = [[i * CORES + c for i in range(chips)] for c in range(CORES)]
        column = lax.all_gather(attended, "tensor", axis=0, tiled=True, axis_index_groups=alike)
        chip_order = list(range(chips))
    if groups <= FEW and groups & (groups - 1) == 0:
        gathered = [column] + [exchange(column, "dp", groups, 1, hop) for hop in range(1, groups)]
        group_order = [group ^ hop for hop in range(groups)]
    else:
        gathered = [lax.all_gather(column, "dp", axis=0, tiled=True)]
        group_order = list(range(groups))

    own = local_weights(new_weight, synced_weight, resident, group.reshape(1), groups)
    other = exchange(own, "tensor", devices, 1, 1)
    owners = jnp.stack(
        [device, device ^ 1]
        + [(g * chips + c) * count + r for g in group_order for c in chip_order for r in range(count)]
    ).astype(jnp.int32)
    partial = project(gathered, own, other, owners, groups * chips * count, steps)
    alike = [
        [g * devices + i * CORES + c for g in range(groups) for i in range(chips)] for c in range(CORES)
    ]
    summed = lax.all_to_all(
        partial, ("dp", "tensor"), split_axis=0, concat_axis=0, tiled=True, axis_index_groups=alike
    )
    return normalise(summed, gain, groups)


def solution(mesh):
    in_specs = (
        P(("dp", "tensor"), None),
        P(("dp", "tensor"), None),
        P(None, "tensor"),
        P(),
        P(("dp", "tensor"), None, None),
        P(("dp", "tensor"), None, None),
        P(("dp", "tensor"), None, None),
        P(("dp", "tensor"), None, None),
        P(("dp", "tensor"), None, None),
        P(("dp", "tensor")),
    )
    out_specs = P(("dp", "tensor"), None, None)
    return jax.shard_map(body, mesh=mesh, in_specs=in_specs, out_specs=out_specs, check_vma=False)
```

```python
import functools

import jax
import jax.numpy as jnp
from jax import lax
from jax.experimental import pallas as pl
from jax.experimental.pallas import tpu as pltpu
from jax.sharding import PartitionSpec as P


HD = 128
CORES = 2
MOST = 32
FEW = 4
NT = (((1,), (1,)), ((), ()))
NN = (((1,), (0,)), ((), ()))


def dot(a, b, dims):
    return lax.dot_general(a, b, dims, preferred_element_type=jnp.float32)


def limit(mebibytes):
    return pltpu.CompilerParams(vmem_limit_bytes=mebibytes << 20)


def held(space, *arrays):
    return [pltpu.with_memory_space_constraint(a, space) for a in arrays]


def divisor(total, most, unit):
    fits = [n for n in range(unit, min(total, most) + 1, unit) if total % n == 0]
    return fits[-1] if fits else total


def attend_kernel(
    length_ref,
    query_ref,
    keys_hbm,
    values_hbm,
    new_keys_ref,
    new_values_ref,
    resident_hbm,
    out_ref,
    cut_hbm,
    keys_ref,
    values_ref,
    past_ref,
    own_ref,
    cut_ref,
    sems,
    *,
    width,
):
    row = pl.program_id(0)
    steps, features = query_ref.shape[1:]
    _, kv_features = keys_ref.shape
    grouping = features // kv_features
    heads = width // HD
    bands = kv_features // width
    block_rows = grouping * steps
    rows = heads * block_rows
    factor = HD ** (-0.5)
    load_keys, load_values = [], []
    for band in range(bands):
        at = pl.ds(band * width, width)
        load_keys.append(pltpu.make_async_copy(keys_hbm.at[row, :, at], keys_ref.at[:, at], sems.at[band]))
        load_values.append(
            pltpu.make_async_copy(values_hbm.at[row, :, at], values_ref.at[:, at], sems.at[bands + band])
        )
    for copy in load_keys + load_values:
        copy.start()
    blocks = cut_hbm.shape[0]
    part = pl.ds(lax.axis_index("dp") * blocks, blocks)
    cut_in = pltpu.make_async_copy(resident_hbm.at[part], cut_ref, sems.at[2 * bands])
    cut_out = pltpu.make_async_copy(cut_ref, cut_hbm, sems.at[2 * bands + 1])
    cut_in.start()

    query = query_ref[0].astype(jnp.float32)
    padding = jnp.zeros((8 - steps % 8, kv_features), jnp.float32)
    keys_new = jnp.concatenate([new_keys_ref[0].astype(jnp.float32), padding], axis=0).astype(jnp.bfloat16)
    values_new = jnp.concatenate([new_values_ref[0].astype(jnp.float32), padding], axis=0).astype(jnp.bfloat16)
    stacks = []
    for band in range(bands):
        lines = []
        for k in range(heads):
            first = (band * heads + k) * grouping
            pieces = [query[:, (first + g) * HD : (first + g + 1) * HD] for g in range(grouping)]
            own = jnp.concatenate(pieces, axis=0)
            lines.append(jnp.concatenate([own if i == k else jnp.zeros_like(own) for i in range(heads)], axis=1))
        stacks.append(jnp.concatenate(lines, axis=0).astype(jnp.bfloat16))
    for band in range(bands):
        at = slice(band * width, (band + 1) * width)
        own_ref[band * rows : (band + 1) * rows] = dot(stacks[band], keys_new[:, at], NT)
    for band in range(bands):
        at = slice(band * width, (band + 1) * width)
        load_keys[band].wait()
        past_ref[band * rows : (band + 1) * rows] = dot(stacks[band], keys_ref[:, at], NT)

    cut_in.wait()
    cut_out.start()
    past = past_ref[...] * factor
    own = own_ref[...] * factor
    slot = lax.broadcasted_iota(jnp.int32, past.shape, 1)
    past = jnp.where(slot < length_ref[row], past, -jnp.inf)
    column = lax.broadcasted_iota(jnp.int32, own.shape, 1)
    position = lax.rem(lax.broadcasted_iota(jnp.int32, own.shape, 0), steps)
    own = jnp.where(column <= position, own, -jnp.inf)
    highest = jnp.maximum(jnp.max(past, axis=1, keepdims=True), jnp.max(own, axis=1, keepdims=True))
    past = jnp.exp(past - highest)
    own = jnp.exp(own - highest)
    scale = 1.0 / (jnp.sum(past, axis=1, keepdims=True) + jnp.sum(own, axis=1, keepdims=True))
    past = (past * scale).astype(jnp.bfloat16)
    own = (own * scale).astype(jnp.bfloat16)

    for band in range(bands):
        at = slice(band * width, (band + 1) * width)
        lines = slice(band * rows, (band + 1) * rows)
        load_values[band].wait()
        attended = dot(past[lines], values_ref[:, at], NN) + dot(own[lines], values_new[:, at], NN)
        for k in range(heads):
            for g in range(grouping):
                head = (band * heads + k) * grouping + g
                piece = k * block_rows + g * steps
                value = attended[piece : piece + steps, k * HD : (k + 1) * HD].astype(jnp.bfloat16)
                for copy in range(out_ref.shape[0]):
                    out_ref[copy, 0, :, head * HD : (head + 1) * HD] = value
    cut_out.wait()


def attend(query, cache_keys, cache_values, new_keys, new_values, cache_lengths, stored, blocks, copies):
    rows, steps, features = query.shape
    slots, kv_features = cache_keys.shape[1:]
    width = HD * 2 if kv_features % (HD * 2) == 0 else HD
    bands = kv_features // width
    lines = features // HD * steps
    one = lambda s: pl.BlockSpec((1, *s[1:]), lambda r, *_: (r, 0, 0))
    hbm = pl.BlockSpec(memory_space=pltpu.HBM)
    return pl.pallas_call(
        functools.partial(attend_kernel, width=width),
        out_shape=[
            jax.ShapeDtypeStruct((copies, *query.shape), jnp.bfloat16),
            jax.ShapeDtypeStruct((blocks, *stored.shape[1:]), stored.dtype),
        ],
        grid_spec=pltpu.PrefetchScalarGridSpec(
            num_scalar_prefetch=1,
            grid=(rows,),
            in_specs=[one(query.shape), hbm, hbm, one(new_keys.shape), one(new_values.shape), hbm],
            out_specs=[pl.BlockSpec((copies, 1, steps, features), lambda r, *_: (0, r, 0, 0)), hbm],
            scratch_shapes=[
                pltpu.VMEM((slots, kv_features), cache_keys.dtype),
                pltpu.VMEM((slots, kv_features), cache_values.dtype),
                pltpu.VMEM((lines, slots), jnp.float32),
                pltpu.VMEM((lines, 8 * (steps // 8 + 1)), jnp.float32),
                pltpu.VMEM((blocks, *stored.shape[1:]), stored.dtype),
                pltpu.SemaphoreType.DMA((2 * bands + 2,)),
            ],
        ),
        compiler_params=limit(16),
        name="attend",
    )(cache_lengths, *held(pltpu.HBM, query, cache_keys, cache_values, new_keys, new_values, stored))


def change_kernel(new_hbm, synced_hbm, out_hbm, new_ref, synced_ref, out_ref, sems, *, take):
    blocks, rows, depth = out_ref.shape
    loads, stores = [], []
    for i in range(rows // take):
        at = pl.ds(i * take, take)
        loads.append(
            (
                pltpu.make_async_copy(new_hbm.at[at], new_ref.at[at], sems.at[3 * i]),
                pltpu.make_async_copy(synced_hbm.at[at], synced_ref.at[at], sems.at[3 * i + 1]),
            )
        )
        stores.append(pltpu.make_async_copy(out_ref.at[:, at], out_hbm.at[:, at], sems.at[3 * i + 2]))
        loads[i][0].start()
        loads[i][1].start()
    for i, pair in enumerate(loads):
        pair[0].wait()
        pair[1].wait()
        at = slice(i * take, (i + 1) * take)
        for b in range(blocks):
            columns = slice(b * depth, (b + 1) * depth)
            out_ref[b, at] = (new_ref[at, columns] - synced_ref[at, columns]).astype(jnp.bfloat16)
        stores[i].start()
    for store in stores:
        store.wait()


def local_change(new_weight, synced_weight, blocks):
    rows, features = new_weight.shape
    take = divisor(rows, 24, 8)
    hbm = pl.BlockSpec(memory_space=pltpu.HBM)
    cut = (blocks, rows, features // blocks)
    return pl.pallas_call(
        functools.partial(change_kernel, take=take),
        out_shape=jax.ShapeDtypeStruct(cut, jnp.bfloat16),
        in_specs=[hbm] * 2,
        out_specs=hbm,
        scratch_shapes=[
            pltpu.VMEM((rows, features), jnp.float32),
            pltpu.VMEM((rows, features), jnp.float32),
            pltpu.VMEM(cut, jnp.bfloat16),
            pltpu.SemaphoreType.DMA((3 * (rows // take),)),
        ],
        compiler_params=limit(24),
        name="local_change",
    )(*held(pltpu.HBM, new_weight, synced_weight))


def project_kernel(*refs, parts):
    gathered = refs[:parts]
    change_ref, *weights_hbm = refs[parts : parts + 4]
    out_ref, weights_ref, rows_ref, sums_ref, sems = refs[parts + 4 :]
    owners, steps, _ = out_ref.shape
    blocks, _, depth = change_ref.shape
    device = lax.axis_index("tensor")
    places = (device, device ^ 1)
    group = lax.axis_index("dp") if parts > 1 else 0
    loads = [pltpu.make_async_copy(weights_hbm[w], weights_ref.at[w], sems.at[w]) for w in range(3)]
    for load in loads:
        load.start()

    pieces = []
    for part in gathered:
        for k in range(part.shape[0]):
            pieces.append(part[k].astype(jnp.float32))
    rows_ref[...] = jnp.concatenate(pieces, axis=0).astype(jnp.bfloat16)

    def of_change(ref):
        value = dot(ref[0], rows_ref[:, :depth], NT)
        for b in range(1, blocks):
            value += dot(ref[b], rows_ref[:, b * depth : (b + 1) * depth], NT)
        return value

    own = of_change(change_ref)
    for source, w in enumerate((0, 1)):
        loads[w].wait()
        rows = rows_ref[:, pl.ds(pl.multiple_of(places[source] * depth, depth), depth)]
        for b in range(blocks):
            value = dot(weights_ref[w, b], rows, NT)
            if source == 0:
                sums_ref[b] = value
            else:
                sums_ref[b] += value
    loads[2].wait()
    other = of_change(weights_ref.at[2])
    sums_ref[places[0]] += own
    sums_ref[places[1]] += other
    sums = jnp.concatenate([sums_ref[b] for b in range(blocks)], axis=0).T
    each = owners // parts
    for k in range(owners):
        owner = (group ^ (k // each)) * each + k % each
        out_ref[owner] = sums[k * steps : (k + 1) * steps]


def project(gathered, weights, owners, steps):
    blocks, width, depth = weights[0].shape
    take = owners if len(gathered) > 1 else divisor(owners, MOST, 1)
    several = owners > take
    whole = pl.BlockSpec(memory_space=pltpu.VMEM)
    cut = lambda s: pl.BlockSpec((take, *s[1:]), lambda i: (i, 0, 0)) if several else whole
    out = jax.ShapeDtypeStruct((owners, steps, blocks * width), jnp.float32)
    return pl.pallas_call(
        functools.partial(project_kernel, parts=len(gathered)),
        out_shape=out,
        grid=(owners // take,),
        in_specs=[*[cut(g.shape) for g in gathered], whole, *[pl.BlockSpec(memory_space=pltpu.HBM)] * 3],
        out_specs=cut(out.shape),
        scratch_shapes=[
            pltpu.VMEM((3, blocks, width, depth), jnp.bfloat16),
            pltpu.VMEM((take * steps, blocks * depth), jnp.bfloat16),
            pltpu.VMEM((blocks, width, take * steps), jnp.float32),
            pltpu.SemaphoreType.DMA((3,)),
        ],
        compiler_params=limit(24 if not several else 40),
        name="project",
    )(
        *(gathered if several else held(pltpu.VMEM, *gathered)),
        *held(pltpu.VMEM, weights[0]),
        *held(pltpu.HBM, *weights[1:]),
    )


def norm_kernel(partial_ref, gain_ref, out_ref, sums_ref, *, groups):
    owners, _, columns = partial_ref.shape
    count = out_ref.shape[0]
    chips = owners // groups // count
    for r in range(count):
        for d in range(groups):
            value = partial_ref[d * chips * count + r]
            for z in range(1, chips):
                value += partial_ref[(d * chips + z) * count + r]
            sums_ref[:, d * columns : (d + 1) * columns] = value
        projected = sums_ref[...]
        mean_square = jnp.mean(projected * projected, axis=1, keepdims=True)
        out_ref[r] = (projected * lax.rsqrt(mean_square + 1e-06) * gain_ref[...]).astype(jnp.bfloat16)


def normalise(partial, gain, groups, count):
    steps, columns = partial.shape[1], partial.shape[2] * groups
    return pl.pallas_call(
        functools.partial(norm_kernel, groups=groups),
        out_shape=jax.ShapeDtypeStruct((count, steps, columns), jnp.bfloat16),
        in_specs=[pl.BlockSpec(memory_space=pltpu.VMEM)] * 2,
        out_specs=pl.BlockSpec(memory_space=pltpu.VMEM),
        scratch_shapes=[pltpu.VMEM((steps, columns), jnp.float32)],
        compiler_params=limit(8),
        name="normalise",
    )(partial, gain.reshape(1, columns))


def body(
    new_weight,
    synced_weight,
    resident,
    gain,
    query,
    cache_keys,
    cache_values,
    new_keys,
    new_values,
    cache_lengths,
):
    groups, devices = lax.axis_size("dp"), lax.axis_size("tensor")
    chips = devices // CORES
    count, steps, features = query.shape

    def exchange(value, axis, size, hop):
        return lax.ppermute(value, axis, [(i, i ^ hop) for i in range(size)])

    stored = resident.reshape(groups * devices, -1, resident.shape[1])
    copies, cut = attend(query, cache_keys, cache_values, new_keys, new_values, cache_lengths, stored, devices, chips)
    column = lax.all_to_all(
        copies.reshape(chips * count, steps, features),
        "tensor",
        split_axis=0,
        concat_axis=0,
        tiled=True,
        axis_index_groups=[[i * CORES + c for i in range(chips)] for c in range(CORES)],
    )
    change = local_change(new_weight, synced_weight, devices)
    weights = [change, cut, exchange(cut, "tensor", devices, 1), exchange(change, "tensor", devices, 1)]
    if groups <= FEW and groups & (groups - 1) == 0:
        gathered = [column]
        for hop in range(1, groups):
            gathered.append(exchange(column, "dp", groups, hop))
    else:
        gathered = [lax.all_gather(column, "dp", axis=0, tiled=True)]
    partial = project(gathered, weights, groups * chips * count, steps)
    summed = lax.all_to_all(
        partial,
        ("dp", "tensor"),
        split_axis=0,
        concat_axis=0,
        tiled=True,
        axis_index_groups=[
            [g * devices + i * CORES + c for g in range(groups) for i in range(chips)] for c in range(CORES)
        ],
    )
    return normalise(summed, gain, groups, count)


def solution(mesh):
    in_specs = (
        P(("dp", "tensor"), None),
        P(("dp", "tensor"), None),
        P(None, "tensor"),
        P(),
        P(("dp", "tensor"), None, None),
        P(("dp", "tensor"), None, None),
        P(("dp", "tensor"), None, None),
        P(("dp", "tensor"), None, None),
        P(("dp", "tensor"), None, None),
        P(("dp", "tensor")),
    )
    out_specs = P(("dp", "tensor"), None, None)
    return jax.shard_map(body, mesh=mesh, in_specs=in_specs, out_specs=out_specs, check_vma=False)
```

```python
import functools

import jax
import jax.numpy as jnp
from jax import lax
from jax.experimental import pallas as pl
from jax.experimental.pallas import tpu as pltpu
from jax.sharding import PartitionSpec as P


HD = 128
CORES = 2
MOST = 32
FEW = 4
NT = (((1,), (1,)), ((), ()))
NN = (((1,), (0,)), ((), ()))


def dot(a, b, dims):
    return lax.dot_general(a, b, dims, preferred_element_type=jnp.float32)


def limit(mebibytes):
    return pltpu.CompilerParams(vmem_limit_bytes=mebibytes << 20)


def held(space, *arrays):
    return [pltpu.with_memory_space_constraint(a, space) for a in arrays]


def divisor(total, most, unit):
    fits = [n for n in range(unit, min(total, most) + 1, unit) if total % n == 0]
    return fits[-1] if fits else total


def attend_kernel(
    lengths_ref,
    query_hbm,
    keys_hbm,
    values_hbm,
    new_keys_hbm,
    new_values_hbm,
    out_hbm,
    query_ref,
    keys_ref,
    values_ref,
    new_keys_ref,
    new_values_ref,
    past_ref,
    own_ref,
    out_ref,
    sems,
    *,
    width,
):
    count, steps, features = query_hbm.shape
    _, kv_features = keys_ref.shape
    grouping = features // kv_features
    heads = width // HD
    bands = kv_features // width
    block_rows = grouping * steps
    rows = heads * block_rows
    factor = HD ** (-0.5)
    for row in range(count):
        pairs = [
            (query_hbm, query_ref),
            (new_keys_hbm, new_keys_ref),
            (keys_hbm, keys_ref),
            (new_values_hbm, new_values_ref),
            (values_hbm, values_ref),
        ]
        loads = [pltpu.make_async_copy(p[0].at[row], p[1], sems.at[i]) for i, p in enumerate(pairs)]
        for load in loads:
            load.start()

        padding = jnp.zeros((8 - steps % 8, kv_features), jnp.float32)
        loads[0].wait()
        query = query_ref[...].astype(jnp.float32)
        stacks = []
        for band in range(bands):
            lines = []
            for k in range(heads):
                first = (band * heads + k) * grouping
                pieces = [query[:, (first + g) * HD : (first + g + 1) * HD] for g in range(grouping)]
                own = jnp.concatenate(pieces, axis=0)
                lines.append(jnp.concatenate([own if i == k else jnp.zeros_like(own) for i in range(heads)], axis=1))
            stacks.append(jnp.concatenate(lines, axis=0).astype(jnp.bfloat16))
        loads[1].wait()
        keys_new = jnp.concatenate([new_keys_ref[...].astype(jnp.float32), padding], axis=0).astype(jnp.bfloat16)
        for band in range(bands):
            at = slice(band * width, (band + 1) * width)
            own_ref[band * rows : (band + 1) * rows] = dot(stacks[band], keys_new[:, at], NT)
        loads[2].wait()
        for band in range(bands):
            at = slice(band * width, (band + 1) * width)
            past_ref[band * rows : (band + 1) * rows] = dot(stacks[band], keys_ref[:, at], NT)

        past = past_ref[...] * factor
        own = own_ref[...] * factor
        slot = lax.broadcasted_iota(jnp.int32, past.shape, 1)
        past = jnp.where(slot < lengths_ref[row], past, -jnp.inf)
        column = lax.broadcasted_iota(jnp.int32, own.shape, 1)
        position = lax.rem(lax.broadcasted_iota(jnp.int32, own.shape, 0), steps)
        own = jnp.where(column <= position, own, -jnp.inf)
        highest = jnp.maximum(jnp.max(past, axis=1, keepdims=True), jnp.max(own, axis=1, keepdims=True))
        past = jnp.exp(past - highest)
        own = jnp.exp(own - highest)
        scale = 1.0 / (jnp.sum(past, axis=1, keepdims=True) + jnp.sum(own, axis=1, keepdims=True))
        past = (past * scale).astype(jnp.bfloat16)
        own = (own * scale).astype(jnp.bfloat16)

        loads[3].wait()
        values_new = jnp.concatenate([new_values_ref[...].astype(jnp.float32), padding], axis=0).astype(jnp.bfloat16)
        loads[4].wait()
        for band in range(bands):
            at = slice(band * width, (band + 1) * width)
            lines = slice(band * rows, (band + 1) * rows)
            attended = dot(past[lines], values_ref[:, at], NN) + dot(own[lines], values_new[:, at], NN)
            for k in range(heads):
                for g in range(grouping):
                    head = (band * heads + k) * grouping + g
                    piece = k * block_rows + g * steps
                    value = attended[piece : piece + steps, k * HD : (k + 1) * HD]
                    out_ref[:, head * HD : (head + 1) * HD] = value.astype(jnp.bfloat16)
        stores = [
            pltpu.make_async_copy(out_ref, out_hbm.at[copy, row], sems.at[5 + copy])
            for copy in range(out_hbm.shape[0])
        ]
        for store in stores:
            store.start()
        for store in stores:
            store.wait()


def attend(query, cache_keys, cache_values, new_keys, new_values, cache_lengths, copies):
    _, steps, features = query.shape
    slots, kv_features = cache_keys.shape[1:]
    width = HD * 2 if kv_features % (HD * 2) == 0 else HD
    lines = features // HD * steps
    hbm = pl.BlockSpec(memory_space=pltpu.HBM)
    operands = held(pltpu.HBM, query, cache_keys, cache_values, new_keys, new_values)
    return pl.pallas_call(
        functools.partial(attend_kernel, width=width),
        out_shape=jax.ShapeDtypeStruct((copies, *query.shape), query.dtype),
        in_specs=[pl.BlockSpec(memory_space=pltpu.SMEM), *[hbm] * len(operands)],
        out_specs=hbm,
        scratch_shapes=[
            *[pltpu.VMEM(o.shape[1:], o.dtype) for o in operands],
            pltpu.VMEM((lines, slots), jnp.float32),
            pltpu.VMEM((lines, 8 * (steps // 8 + 1)), jnp.float32),
            pltpu.VMEM(query.shape[1:], query.dtype),
            pltpu.SemaphoreType.DMA((5 + copies,)),
        ],
        compiler_params=limit(16),
        name="attend",
    )(cache_lengths, *operands)


def change_kernel(new_hbm, synced_hbm, out_hbm, new_ref, synced_ref, out_ref, sems, *, take):
    blocks, rows, depth = out_ref.shape
    loads, stores = [], []
    for i in range(rows // take):
        at = pl.ds(i * take, take)
        loads.append(
            (
                pltpu.make_async_copy(new_hbm.at[at], new_ref.at[at], sems.at[3 * i]),
                pltpu.make_async_copy(synced_hbm.at[at], synced_ref.at[at], sems.at[3 * i + 1]),
            )
        )
        stores.append(pltpu.make_async_copy(out_ref.at[:, at], out_hbm.at[:, at], sems.at[3 * i + 2]))
        loads[i][0].start()
        loads[i][1].start()
    for i, pair in enumerate(loads):
        pair[0].wait()
        pair[1].wait()
        at = slice(i * take, (i + 1) * take)
        for b in range(blocks):
            columns = slice(b * depth, (b + 1) * depth)
            out_ref[b, at] = (new_ref[at, columns] - synced_ref[at, columns]).astype(jnp.bfloat16)
        stores[i].start()
    for store in stores:
        store.wait()


def local_change(new_weight, synced_weight, blocks):
    rows, features = new_weight.shape
    take = divisor(rows, 24, 8)
    hbm = pl.BlockSpec(memory_space=pltpu.HBM)
    cut = (blocks, rows, features // blocks)
    return pl.pallas_call(
        functools.partial(change_kernel, take=take),
        out_shape=jax.ShapeDtypeStruct(cut, jnp.bfloat16),
        in_specs=[hbm] * 2,
        out_specs=hbm,
        scratch_shapes=[
            pltpu.VMEM((rows, features), jnp.float32),
            pltpu.VMEM((rows, features), jnp.float32),
            pltpu.VMEM(cut, jnp.bfloat16),
            pltpu.SemaphoreType.DMA((3 * (rows // take),)),
        ],
        compiler_params=limit(24),
        name="local_change",
    )(*held(pltpu.HBM, new_weight, synced_weight))


def fetch_kernel(own_hbm, other_hbm, own_ref, other_ref, sems):
    blocks = own_ref.shape[0]
    part = pl.ds(lax.axis_index("dp") * blocks, blocks)
    loads = [
        pltpu.make_async_copy(own_hbm.at[part], own_ref, sems.at[0]),
        pltpu.make_async_copy(other_hbm.at[part], other_ref, sems.at[1]),
    ]
    for load in loads:
        load.start()
    for load in loads:
        load.wait()


def fetch(own, other, blocks):
    cut = (blocks, *own.shape[1:])
    return pl.pallas_call(
        fetch_kernel,
        out_shape=[pltpu.VMEM(cut, own.dtype)] * 2,
        in_specs=[pl.BlockSpec(memory_space=pltpu.HBM)] * 2,
        out_specs=[pl.BlockSpec(memory_space=pltpu.VMEM)] * 2,
        scratch_shapes=[pltpu.SemaphoreType.DMA((2,))],
        compiler_params=limit(8),
        name="fetch",
    )(*held(pltpu.HBM, own, other))


def project_kernel(*refs, parts):
    gathered = refs[:parts]
    own_ref, other_ref, own_change_ref, other_change_ref = refs[parts : parts + 4]
    out_ref, rows_ref, sums_ref = refs[parts + 4 :]
    owners, steps, _ = out_ref.shape
    blocks, _, depth = own_ref.shape
    device = lax.axis_index("tensor")
    places = (device, device ^ 1)
    group = lax.axis_index("dp")

    pieces = []
    for part in gathered:
        for k in range(part.shape[0]):
            pieces.append(part[k].astype(jnp.float32))
    rows_ref[...] = jnp.concatenate(pieces, axis=0).astype(jnp.bfloat16)

    for source, ref in enumerate((own_ref, other_ref)):
        rows = rows_ref[:, pl.ds(pl.multiple_of(places[source] * depth, depth), depth)]
        for b in range(blocks):
            value = dot(ref[b], rows, NT)
            if source == 0:
                sums_ref[b] = value
            else:
                sums_ref[b] += value
    for source, ref in enumerate((own_change_ref, other_change_ref)):
        value = dot(ref[0], rows_ref[:, :depth], NT)
        for b in range(1, blocks):
            value += dot(ref[b], rows_ref[:, b * depth : (b + 1) * depth], NT)
        sums_ref[places[source]] += value
    sums = jnp.concatenate([sums_ref[b] for b in range(blocks)], axis=0).T
    each = owners // parts
    for k in range(owners):
        owner = (group ^ (k // each)) * each + k % each if parts > 1 else k
        out_ref[owner] = sums[k * steps : (k + 1) * steps]


def project(gathered, weights, owners, steps):
    blocks, width, depth = weights[0].shape
    take = owners if len(gathered) > 1 else divisor(owners, MOST, 1)
    several = owners > take
    whole = pl.BlockSpec(memory_space=pltpu.VMEM)
    cut = lambda s: pl.BlockSpec((take, *s[1:]), lambda i: (i, 0, 0)) if several else whole
    out = jax.ShapeDtypeStruct((owners, steps, blocks * width), jnp.float32)
    return pl.pallas_call(
        functools.partial(project_kernel, parts=len(gathered)),
        out_shape=out,
        grid=(owners // take,),
        in_specs=[*[cut(g.shape) for g in gathered], *[whole] * 4],
        out_specs=cut(out.shape),
        scratch_shapes=[
            pltpu.VMEM((take * steps, blocks * depth), jnp.bfloat16),
            pltpu.VMEM((blocks, width, take * steps), jnp.float32),
        ],
        compiler_params=limit(24 if not several else 40),
        name="project",
    )(
        *(gathered if several else held(pltpu.VMEM, *gathered)),
        *held(pltpu.VMEM, *weights),
    )


def norm_kernel(partial_ref, gain_ref, out_ref, sums_ref, *, groups):
    owners, _, columns = partial_ref.shape
    count = out_ref.shape[0]
    chips = owners // groups // count
    for r in range(count):
        for d in range(groups):
            value = partial_ref[d * chips * count + r]
            for z in range(1, chips):
                value += partial_ref[(d * chips + z) * count + r]
            sums_ref[:, d * columns : (d + 1) * columns] = value
        projected = sums_ref[...]
        mean_square = jnp.mean(projected * projected, axis=1, keepdims=True)
        out_ref[r] = (projected * lax.rsqrt(mean_square + 1e-06) * gain_ref[...]).astype(jnp.bfloat16)


def normalise(partial, gain, groups, count):
    steps, columns = partial.shape[1], partial.shape[2] * groups
    return pl.pallas_call(
        functools.partial(norm_kernel, groups=groups),
        out_shape=jax.ShapeDtypeStruct((count, steps, columns), jnp.bfloat16),
        in_specs=[pl.BlockSpec(memory_space=pltpu.VMEM)] * 2,
        out_specs=pl.BlockSpec(memory_space=pltpu.VMEM),
        scratch_shapes=[pltpu.VMEM((steps, columns), jnp.float32)],
        compiler_params=limit(8),
        name="normalise",
    )(partial, gain.reshape(1, columns))


def body(
    new_weight,
    synced_weight,
    resident,
    gain,
    query,
    cache_keys,
    cache_values,
    new_keys,
    new_values,
    cache_lengths,
):
    groups, devices = lax.axis_size("dp"), lax.axis_size("tensor")
    chips = devices // CORES
    count, steps, features = query.shape

    def exchange(value, axis, size, hop):
        return lax.ppermute(value, axis, [(i, i ^ hop) for i in range(size)])

    stored = resident.reshape(groups * devices, -1, resident.shape[1])
    copies = attend(query, cache_keys, cache_values, new_keys, new_values, cache_lengths, chips)
    column = lax.all_to_all(
        copies.reshape(chips * count, steps, features),
        "tensor",
        split_axis=0,
        concat_axis=0,
        tiled=True,
        axis_index_groups=[[i * CORES + c for i in range(chips)] for c in range(CORES)],
    )
    change = local_change(new_weight, synced_weight, devices)
    other = exchange(stored, "tensor", devices, 1)
    column, later = lax.optimization_barrier((column, change))
    other_change = exchange(later, "tensor", devices, 1)
    if groups <= FEW and groups & (groups - 1) == 0:
        gathered = [column]
        for hop in range(1, groups):
            gathered.append(exchange(column, "dp", groups, hop))
    else:
        gathered = [lax.all_gather(column, "dp", axis=0, tiled=True)]
    near = fetch(stored, other, devices)
    partial = project(gathered, [*near, change, other_change], groups * chips * count, steps)
    summed = lax.all_to_all(
        partial,
        ("dp", "tensor"),
        split_axis=0,
        concat_axis=0,
        tiled=True,
        axis_index_groups=[
            [g * devices + i * CORES + c for g in range(groups) for i in range(chips)] for c in range(CORES)
        ],
    )
    return normalise(summed, gain, groups, count)


def solution(mesh):
    in_specs = (
        P(("dp", "tensor"), None),
        P(("dp", "tensor"), None),
        P(None, "tensor"),
        P(),
        P(("dp", "tensor"), None, None),
        P(("dp", "tensor"), None, None),
        P(("dp", "tensor"), None, None),
        P(("dp", "tensor"), None, None),
        P(("dp", "tensor"), None, None),
        P(("dp", "tensor")),
    )
    out_specs = P(("dp", "tensor"), None, None)
    return jax.shard_map(body, mesh=mesh, in_specs=in_specs, out_specs=out_specs, check_vma=False)
```

```python
import functools

import jax
import jax.numpy as jnp
from jax import lax
from jax.experimental import pallas as pl
from jax.experimental.pallas import tpu as pltpu
from jax.sharding import PartitionSpec as P


HD = 128
CORES = 2
MOST = 32
FEW = 4
NT = (((1,), (1,)), ((), ()))
NN = (((1,), (0,)), ((), ()))


def dot(a, b, dims):
    return lax.dot_general(a, b, dims, preferred_element_type=jnp.float32)


def limit(mebibytes):
    return pltpu.CompilerParams(vmem_limit_bytes=mebibytes << 20)


def held(space, *arrays):
    return [pltpu.with_memory_space_constraint(a, space) for a in arrays]


def divisor(total, most, unit):
    fits = [n for n in range(unit, min(total, most) + 1, unit) if total % n == 0]
    return fits[-1] if fits else total


def attend_kernel(
    lengths_ref,
    query_hbm,
    keys_hbm,
    values_hbm,
    new_keys_hbm,
    new_values_hbm,
    resident_hbm,
    out_ref,
    near_ref,
    query_ref,
    keys_ref,
    values_ref,
    new_keys_ref,
    new_values_ref,
    past_ref,
    own_ref,
    sems,
    *,
    width,
):
    count, steps, features = query_hbm.shape
    _, kv_features = keys_ref.shape
    grouping = features // kv_features
    heads = width // HD
    bands = kv_features // width
    block_rows = grouping * steps
    rows = heads * block_rows
    factor = HD ** (-0.5)
    blocks = near_ref.shape[0]
    near = pltpu.make_async_copy(resident_hbm.at[pl.ds(lax.axis_index("dp") * blocks, blocks)], near_ref, sems.at[5])
    for row in range(count):
        pairs = [
            (query_hbm, query_ref),
            (new_keys_hbm, new_keys_ref),
            (keys_hbm, keys_ref),
            (new_values_hbm, new_values_ref),
            (values_hbm, values_ref),
        ]
        loads = [pltpu.make_async_copy(p[0].at[row], p[1], sems.at[i]) for i, p in enumerate(pairs)]
        for load in loads:
            load.start()
        if row == 0:
            near.start()

        padding = jnp.zeros((8 - steps % 8, kv_features), jnp.float32)
        loads[0].wait()
        query = query_ref[...].astype(jnp.float32)
        stacks = []
        for band in range(bands):
            lines = []
            for k in range(heads):
                first = (band * heads + k) * grouping
                pieces = [query[:, (first + g) * HD : (first + g + 1) * HD] for g in range(grouping)]
                own = jnp.concatenate(pieces, axis=0)
                lines.append(jnp.concatenate([own if i == k else jnp.zeros_like(own) for i in range(heads)], axis=1))
            stacks.append(jnp.concatenate(lines, axis=0).astype(jnp.bfloat16))
        loads[1].wait()
        keys_new = jnp.concatenate([new_keys_ref[...].astype(jnp.float32), padding], axis=0).astype(jnp.bfloat16)
        for band in range(bands):
            at = slice(band * width, (band + 1) * width)
            own_ref[band * rows : (band + 1) * rows] = dot(stacks[band], keys_new[:, at], NT)
        loads[2].wait()
        for band in range(bands):
            at = slice(band * width, (band + 1) * width)
            past_ref[band * rows : (band + 1) * rows] = dot(stacks[band], keys_ref[:, at], NT)

        past = past_ref[...] * factor
        own = own_ref[...] * factor
        slot = lax.broadcasted_iota(jnp.int32, past.shape, 1)
        past = jnp.where(slot < lengths_ref[row], past, -jnp.inf)
        column = lax.broadcasted_iota(jnp.int32, own.shape, 1)
        position = lax.rem(lax.broadcasted_iota(jnp.int32, own.shape, 0), steps)
        own = jnp.where(column <= position, own, -jnp.inf)
        highest = jnp.maximum(jnp.max(past, axis=1, keepdims=True), jnp.max(own, axis=1, keepdims=True))
        past = jnp.exp(past - highest)
        own = jnp.exp(own - highest)
        scale = 1.0 / (jnp.sum(past, axis=1, keepdims=True) + jnp.sum(own, axis=1, keepdims=True))
        past = (past * scale).astype(jnp.bfloat16)
        own = (own * scale).astype(jnp.bfloat16)

        loads[3].wait()
        values_new = jnp.concatenate([new_values_ref[...].astype(jnp.float32), padding], axis=0).astype(jnp.bfloat16)
        loads[4].wait()
        for band in range(bands):
            at = slice(band * width, (band + 1) * width)
            lines = slice(band * rows, (band + 1) * rows)
            attended = dot(past[lines], values_ref[:, at], NN) + dot(own[lines], values_new[:, at], NN)
            for k in range(heads):
                for g in range(grouping):
                    head = (band * heads + k) * grouping + g
                    piece = k * block_rows + g * steps
                    value = attended[piece : piece + steps, k * HD : (k + 1) * HD]
                    out_ref[row, :, head * HD : (head + 1) * HD] = value.astype(jnp.bfloat16)
    near.wait()


def attend(query, cache_keys, cache_values, new_keys, new_values, cache_lengths, stored, blocks):
    _, steps, features = query.shape
    slots, kv_features = cache_keys.shape[1:]
    width = HD * 2 if kv_features % (HD * 2) == 0 else HD
    lines = features // HD * steps
    hbm = pl.BlockSpec(memory_space=pltpu.HBM)
    operands = held(pltpu.HBM, query, cache_keys, cache_values, new_keys, new_values)
    return pl.pallas_call(
        functools.partial(attend_kernel, width=width),
        out_shape=[pltpu.VMEM(query.shape, query.dtype), pltpu.VMEM((blocks, *stored.shape[1:]), stored.dtype)],
        in_specs=[pl.BlockSpec(memory_space=pltpu.SMEM), *[hbm] * (len(operands) + 1)],
        out_specs=[pl.BlockSpec(memory_space=pltpu.VMEM)] * 2,
        scratch_shapes=[
            *[pltpu.VMEM(o.shape[1:], o.dtype) for o in operands],
            pltpu.VMEM((lines, slots), jnp.float32),
            pltpu.VMEM((lines, 8 * (steps // 8 + 1)), jnp.float32),
            pltpu.SemaphoreType.DMA((6,)),
        ],
        compiler_params=limit(16),
        name="attend",
    )(cache_lengths, *operands, *held(pltpu.HBM, stored))


def join_kernel(*refs):
    *part_refs, out_ref = refs
    count = part_refs[0].shape[0]
    for i, ref in enumerate(part_refs):
        out_ref[i * count : (i + 1) * count] = ref[...]


def join(parts):
    whole = pl.BlockSpec(memory_space=pltpu.VMEM)
    count = parts[0].shape[0]
    return pl.pallas_call(
        join_kernel,
        out_shape=pltpu.VMEM((count * len(parts), *parts[0].shape[1:]), parts[0].dtype),
        in_specs=[whole] * len(parts),
        out_specs=whole,
        compiler_params=limit(4),
        name="join",
    )(*held(pltpu.VMEM, *parts))


def change_kernel(new_hbm, synced_hbm, out_ref, new_ref, synced_ref, sems, *, first, take):
    blocks, rows, depth = out_ref.shape
    loads = []
    for i in range(rows // take):
        at, near = pl.ds(first + i * take, take), pl.ds(i * take, take)
        loads.append(
            (
                pltpu.make_async_copy(new_hbm.at[at], new_ref.at[near], sems.at[2 * i]),
                pltpu.make_async_copy(synced_hbm.at[at], synced_ref.at[near], sems.at[2 * i + 1]),
            )
        )
        loads[i][0].start()
        loads[i][1].start()
    for i, pair in enumerate(loads):
        pair[0].wait()
        pair[1].wait()
        at = slice(i * take, (i + 1) * take)
        for b in range(blocks):
            columns = slice(b * depth, (b + 1) * depth)
            out_ref[b, at] = (new_ref[at, columns] - synced_ref[at, columns]).astype(jnp.bfloat16)


def local_change(new_weight, synced_weight, blocks, first, rows, take):
    features = new_weight.shape[1]
    return pl.pallas_call(
        functools.partial(change_kernel, first=first, take=take),
        out_shape=pltpu.VMEM((blocks, rows, features // blocks), jnp.bfloat16),
        in_specs=[pl.BlockSpec(memory_space=pltpu.HBM)] * 2,
        out_specs=pl.BlockSpec(memory_space=pltpu.VMEM),
        scratch_shapes=[
            pltpu.VMEM((rows, features), jnp.float32),
            pltpu.VMEM((rows, features), jnp.float32),
            pltpu.SemaphoreType.DMA((2 * (rows // take),)),
        ],
        compiler_params=limit(14),
        name="local_change",
    )(*held(pltpu.HBM, new_weight, synced_weight))


def project_kernel(*refs, parts, cuts):
    gathered, refs = refs[:parts], refs[parts:]
    changes, (own_ref, other_ref, out_ref, rows_ref, sums_ref) = refs[: 2 * cuts], refs[2 * cuts :]
    owners, steps, _ = out_ref.shape
    blocks, _, depth = own_ref.shape
    device = lax.axis_index("tensor")
    places = (device, device ^ 1)
    group, chip = lax.axis_index("dp"), device // CORES

    pieces = []
    for part in gathered:
        for k in range(part.shape[0]):
            pieces.append(part[k].astype(jnp.float32))
    rows_ref[...] = jnp.concatenate(pieces, axis=0).astype(jnp.bfloat16)

    deltas = []
    for ref in changes:
        value = dot(ref[0], rows_ref[:, :depth], NT)
        for b in range(1, blocks):
            value += dot(ref[b], rows_ref[:, b * depth : (b + 1) * depth], NT)
        deltas.append(value)
    for source, ref in enumerate((own_ref, other_ref)):
        rows = rows_ref[:, pl.ds(pl.multiple_of(places[source] * depth, depth), depth)]
        for b in range(blocks):
            value = dot(ref[b], rows, NT)
            if source == 0:
                sums_ref[b] = value
            else:
                sums_ref[b] += value
    for source in range(2):
        first = 0
        for value in deltas[source * cuts : (source + 1) * cuts]:
            sums_ref[places[source], first : first + value.shape[0]] += value
            first += value.shape[0]
    sums = jnp.concatenate([sums_ref[b] for b in range(blocks)], axis=0).T
    each = owners // parts
    for k in range(owners):
        owner = k
        if parts > 1:
            chips = device_count() // CORES
            count = each // chips
            hop, r = k % each // count, k % count
            owner = ((group ^ (k // each)) * chips + (chip ^ hop)) * count + r
        out_ref[owner] = sums[k * steps : (k + 1) * steps]


def device_count():
    return lax.axis_size("tensor")


def project(gathered, changes, own, other, owners, steps):
    blocks, width, depth = own.shape
    take = owners if len(gathered) > 1 else divisor(owners, MOST, 1)
    several = owners > take
    whole = pl.BlockSpec(memory_space=pltpu.VMEM)
    cut = lambda s: pl.BlockSpec((take, *s[1:]), lambda i: (i, 0, 0)) if several else whole
    out = jax.ShapeDtypeStruct((owners, steps, blocks * width), jnp.float32)
    return pl.pallas_call(
        functools.partial(project_kernel, parts=len(gathered), cuts=len(changes) // 2),
        out_shape=out,
        grid=(owners // take,),
        in_specs=[*[cut(g.shape) for g in gathered], *[whole] * (len(changes) + 2)],
        out_specs=cut(out.shape),
        scratch_shapes=[
            pltpu.VMEM((take * steps, blocks * depth), jnp.bfloat16),
            pltpu.VMEM((blocks, width, take * steps), jnp.float32),
        ],
        compiler_params=limit(16 if not several else 40),
        name="project",
    )(
        *(gathered if several else held(pltpu.VMEM, *gathered)),
        *held(pltpu.VMEM, *changes, own, other),
    )


def norm_kernel(partial_ref, gain_ref, out_ref, sums_ref, *, groups):
    owners, _, columns = partial_ref.shape
    count = out_ref.shape[0]
    chips = owners // groups // count
    for r in range(count):
        for d in range(groups):
            value = partial_ref[d * chips * count + r]
            for z in range(1, chips):
                value += partial_ref[(d * chips + z) * count + r]
            sums_ref[:, d * columns : (d + 1) * columns] = value
        projected = sums_ref[...]
        mean_square = jnp.mean(projected * projected, axis=1, keepdims=True)
        out_ref[r] = (projected * lax.rsqrt(mean_square + 1e-06) * gain_ref[...]).astype(jnp.bfloat16)


def normalise(partial, gain, groups, count):
    steps, columns = partial.shape[1], partial.shape[2] * groups
    return pl.pallas_call(
        functools.partial(norm_kernel, groups=groups),
        out_shape=jax.ShapeDtypeStruct((count, steps, columns), jnp.bfloat16),
        in_specs=[pl.BlockSpec(memory_space=pltpu.VMEM)] * 2,
        out_specs=pl.BlockSpec(memory_space=pltpu.VMEM),
        scratch_shapes=[pltpu.VMEM((steps, columns), jnp.float32)],
        compiler_params=limit(8),
        name="normalise",
    )(partial, gain.reshape(1, columns))


def body(
    new_weight,
    synced_weight,
    resident,
    gain,
    query,
    cache_keys,
    cache_values,
    new_keys,
    new_values,
    cache_lengths,
):
    groups, devices = lax.axis_size("dp"), lax.axis_size("tensor")
    chips = devices // CORES
    count, steps, _ = query.shape

    def exchange(value, axis, size, unit, hop):
        return lax.ppermute(value, axis, [(i, (i // unit ^ hop) * unit + i % unit) for i in range(size)])

    def fits(size):
        return size <= FEW and size & (size - 1) == 0

    rows = new_weight.shape[0]
    take = divisor(rows, 24, 8)
    early = (rows // take - rows // take // 3) * take
    stored = resident.reshape(groups * devices, rows, resident.shape[1])
    attended, own_rows = attend(query, cache_keys, cache_values, new_keys, new_values, cache_lengths, stored, devices)
    other_rows = exchange(own_rows, "tensor", devices, 1, 1)
    near = fits(chips) and fits(groups)
    if near:
        column = [attended]
        for hop in range(1, chips):
            column.append(exchange(attended, "tensor", devices, CORES, hop))
        column = join(column)
    else:
        alike = [[i * CORES + c for i in range(chips)] for c in range(CORES)]
        column = lax.all_gather(attended, "tensor", axis=0, tiled=True, axis_index_groups=alike)
    if near:
        gathered = [column]
        for hop in range(1, groups):
            gathered.append(exchange(column, "dp", groups, 1, hop))
    else:
        gathered = [lax.all_gather(column, "dp", axis=0, tiled=True)]
    own, swapped = [], []
    for first, size in ((0, early), (early, rows - early)):
        if size:
            own.append(local_change(new_weight, synced_weight, devices, first, size, take))
            swapped.append(exchange(own[-1], "tensor", devices, 1, 1))
    partial = project(gathered, own + swapped, own_rows, other_rows, groups * chips * count, steps)
    summed = lax.all_to_all(
        partial,
        ("dp", "tensor"),
        split_axis=0,
        concat_axis=0,
        tiled=True,
        axis_index_groups=[
            [g * devices + i * CORES + c for g in range(groups) for i in range(chips)] for c in range(CORES)
        ],
    )
    return normalise(summed, gain, groups, count)


def solution(mesh):
    in_specs = (
        P(("dp", "tensor"), None),
        P(("dp", "tensor"), None),
        P(None, "tensor"),
        P(),
        P(("dp", "tensor"), None, None),
        P(("dp", "tensor"), None, None),
        P(("dp", "tensor"), None, None),
        P(("dp", "tensor"), None, None),
        P(("dp", "tensor"), None, None),
        P(("dp", "tensor")),
    )
    out_specs = P(("dp", "tensor"), None, None)
    return jax.shard_map(body, mesh=mesh, in_specs=in_specs, out_specs=out_specs, check_vma=False)
```

```python
import functools

import jax
import jax.numpy as jnp
from jax import lax
from jax.experimental import pallas as pl
from jax.experimental.pallas import tpu as pltpu
from jax.sharding import PartitionSpec as P


HD = 128
CORES = 2
MOST = 32
FEW = 4
NT = (((1,), (1,)), ((), ()))
NN = (((1,), (0,)), ((), ()))


def dot(a, b, dims):
    return lax.dot_general(a, b, dims, preferred_element_type=jnp.float32)


def limit(mebibytes):
    return pltpu.CompilerParams(vmem_limit_bytes=mebibytes << 20)


def held(space, *arrays):
    return [pltpu.with_memory_space_constraint(a, space) for a in arrays]


def divisor(total, most, unit):
    fits = [n for n in range(unit, min(total, most) + 1, unit) if total % n == 0]
    return fits[-1] if fits else total


def attend_kernel(
    lengths_ref,
    query_hbm,
    keys_hbm,
    values_hbm,
    new_keys_hbm,
    new_values_hbm,
    resident_hbm,
    out_ref,
    near_ref,
    query_ref,
    keys_ref,
    values_ref,
    new_keys_ref,
    new_values_ref,
    past_ref,
    own_ref,
    sems,
    *,
    width,
):
    count, steps, features = query_hbm.shape
    _, kv_features = keys_ref.shape
    grouping = features // kv_features
    heads = width // HD
    bands = kv_features // width
    block_rows = grouping * steps
    rows = heads * block_rows
    factor = HD ** (-0.5)
    blocks = near_ref.shape[0]
    near = pltpu.make_async_copy(resident_hbm.at[pl.ds(lax.axis_index("dp") * blocks, blocks)], near_ref, sems.at[5])
    for row in range(count):
        pairs = [
            (query_hbm, query_ref),
            (new_keys_hbm, new_keys_ref),
            (keys_hbm, keys_ref),
            (new_values_hbm, new_values_ref),
            (values_hbm, values_ref),
        ]
        loads = [pltpu.make_async_copy(p[0].at[row], p[1], sems.at[i]) for i, p in enumerate(pairs)]
        for load in loads:
            load.start()
        if row == 0:
            near.start()

        padding = jnp.zeros((8 - steps % 8, kv_features), jnp.float32)
        loads[0].wait()
        query = query_ref[...].astype(jnp.float32)
        stacks = []
        for band in range(bands):
            lines = []
            for k in range(heads):
                first = (band * heads + k) * grouping
                pieces = [query[:, (first + g) * HD : (first + g + 1) * HD] for g in range(grouping)]
                own = jnp.concatenate(pieces, axis=0)
                lines.append(jnp.concatenate([own if i == k else jnp.zeros_like(own) for i in range(heads)], axis=1))
            stacks.append(jnp.concatenate(lines, axis=0).astype(jnp.bfloat16))
        loads[1].wait()
        keys_new = jnp.concatenate([new_keys_ref[...].astype(jnp.float32), padding], axis=0).astype(jnp.bfloat16)
        for band in range(bands):
            at = slice(band * width, (band + 1) * width)
            own_ref[band * rows : (band + 1) * rows] = dot(stacks[band], keys_new[:, at], NT)
        loads[2].wait()
        for band in range(bands):
            at = slice(band * width, (band + 1) * width)
            past_ref[band * rows : (band + 1) * rows] = dot(stacks[band], keys_ref[:, at], NT)

        past = past_ref[...] * factor
        own = own_ref[...] * factor
        slot = lax.broadcasted_iota(jnp.int32, past.shape, 1)
        past = jnp.where(slot < lengths_ref[row], past, -jnp.inf)
        column = lax.broadcasted_iota(jnp.int32, own.shape, 1)
        position = lax.rem(lax.broadcasted_iota(jnp.int32, own.shape, 0), steps)
        own = jnp.where(column <= position, own, -jnp.inf)
        highest = jnp.maximum(jnp.max(past, axis=1, keepdims=True), jnp.max(own, axis=1, keepdims=True))
        past = jnp.exp(past - highest)
        own = jnp.exp(own - highest)
        scale = 1.0 / (jnp.sum(past, axis=1, keepdims=True) + jnp.sum(own, axis=1, keepdims=True))
        past = (past * scale).astype(jnp.bfloat16)
        own = (own * scale).astype(jnp.bfloat16)

        loads[3].wait()
        values_new = jnp.concatenate([new_values_ref[...].astype(jnp.float32), padding], axis=0).astype(jnp.bfloat16)
        loads[4].wait()
        for band in range(bands):
            at = slice(band * width, (band + 1) * width)
            lines = slice(band * rows, (band + 1) * rows)
            attended = dot(past[lines], values_ref[:, at], NN) + dot(own[lines], values_new[:, at], NN)
            for k in range(heads):
                for g in range(grouping):
                    head = (band * heads + k) * grouping + g
                    piece = k * block_rows + g * steps
                    value = attended[piece : piece + steps, k * HD : (k + 1) * HD]
                    out_ref[row, :, head * HD : (head + 1) * HD] = value.astype(jnp.bfloat16)
    near.wait()


def attend(query, cache_keys, cache_values, new_keys, new_values, cache_lengths, stored, blocks):
    _, steps, features = query.shape
    slots, kv_features = cache_keys.shape[1:]
    width = HD * 2 if kv_features % (HD * 2) == 0 else HD
    lines = features // HD * steps
    hbm = pl.BlockSpec(memory_space=pltpu.HBM)
    operands = held(pltpu.HBM, query, cache_keys, cache_values, new_keys, new_values)
    return pl.pallas_call(
        functools.partial(attend_kernel, width=width),
        out_shape=[pltpu.VMEM(query.shape, query.dtype), pltpu.VMEM((blocks, *stored.shape[1:]), stored.dtype)],
        in_specs=[pl.BlockSpec(memory_space=pltpu.SMEM), *[hbm] * (len(operands) + 1)],
        out_specs=[pl.BlockSpec(memory_space=pltpu.VMEM)] * 2,
        scratch_shapes=[
            *[pltpu.VMEM(o.shape[1:], o.dtype) for o in operands],
            pltpu.VMEM((lines, slots), jnp.float32),
            pltpu.VMEM((lines, 8 * (steps // 8 + 1)), jnp.float32),
            pltpu.SemaphoreType.DMA((6,)),
        ],
        compiler_params=limit(16),
        name="attend",
    )(cache_lengths, *operands, *held(pltpu.HBM, stored))


def join_kernel(*refs):
    *part_refs, out_ref = refs
    count = part_refs[0].shape[0]
    for i, ref in enumerate(part_refs):
        out_ref[i * count : (i + 1) * count] = ref[...]


def join(parts):
    whole = pl.BlockSpec(memory_space=pltpu.VMEM)
    count = parts[0].shape[0]
    return pl.pallas_call(
        join_kernel,
        out_shape=pltpu.VMEM((count * len(parts), *parts[0].shape[1:]), parts[0].dtype),
        in_specs=[whole] * len(parts),
        out_specs=whole,
        compiler_params=limit(4),
        name="join",
    )(*held(pltpu.VMEM, *parts))


def change_kernel(new_ref, synced_ref, out_ref):
    blocks, _, depth = out_ref.shape
    for b in range(blocks):
        columns = slice(b * depth, (b + 1) * depth)
        out_ref[b] = (new_ref[:, columns] - synced_ref[:, columns]).astype(jnp.bfloat16)


def local_change(new_weight, synced_weight, blocks):
    rows, features = new_weight.shape
    whole = pl.BlockSpec(memory_space=pltpu.VMEM)
    return pl.pallas_call(
        change_kernel,
        out_shape=pltpu.VMEM((blocks, rows, features // blocks), jnp.bfloat16),
        in_specs=[whole] * 2,
        out_specs=whole,
        compiler_params=limit(4),
        name="local_change",
    )(*held(pltpu.VMEM, new_weight, synced_weight))


def project_kernel(*refs, parts, cuts):
    gathered, refs = refs[:parts], refs[parts:]
    changes, (own_ref, other_ref, out_ref, rows_ref, sums_ref) = refs[: 2 * cuts], refs[2 * cuts :]
    owners, steps, _ = out_ref.shape
    blocks, _, depth = own_ref.shape
    device = lax.axis_index("tensor")
    places = (device, device ^ 1)
    group, chip = lax.axis_index("dp"), device // CORES

    pieces = []
    for part in gathered:
        for k in range(part.shape[0]):
            pieces.append(part[k].astype(jnp.float32))
    rows_ref[...] = jnp.concatenate(pieces, axis=0).astype(jnp.bfloat16)

    deltas = []
    for ref in changes:
        value = dot(ref[0], rows_ref[:, :depth], NT)
        for b in range(1, blocks):
            value += dot(ref[b], rows_ref[:, b * depth : (b + 1) * depth], NT)
        deltas.append(value)
    for source, ref in enumerate((own_ref, other_ref)):
        rows = rows_ref[:, pl.ds(pl.multiple_of(places[source] * depth, depth), depth)]
        for b in range(blocks):
            value = dot(ref[b], rows, NT)
            if source == 0:
                sums_ref[b] = value
            else:
                sums_ref[b] += value
    for source in range(2):
        first = 0
        for value in deltas[source * cuts : (source + 1) * cuts]:
            sums_ref[places[source], first : first + value.shape[0]] += value
            first += value.shape[0]
    sums = jnp.concatenate([sums_ref[b] for b in range(blocks)], axis=0).T
    each = owners // parts
    for k in range(owners):
        owner = k
        if parts > 1:
            chips = device_count() // CORES
            count = each // chips
            hop, r = k % each // count, k % count
            owner = ((group ^ (k // each)) * chips + (chip ^ hop)) * count + r
        out_ref[owner] = sums[k * steps : (k + 1) * steps]


def device_count():
    return lax.axis_size("tensor")


def project(gathered, changes, own, other, owners, steps):
    blocks, width, depth = own.shape
    take = owners if len(gathered) > 1 else divisor(owners, MOST, 1)
    several = owners > take
    whole = pl.BlockSpec(memory_space=pltpu.VMEM)
    cut = lambda s: pl.BlockSpec((take, *s[1:]), lambda i: (i, 0, 0)) if several else whole
    out = jax.ShapeDtypeStruct((owners, steps, blocks * width), jnp.float32)
    return pl.pallas_call(
        functools.partial(project_kernel, parts=len(gathered), cuts=len(changes) // 2),
        out_shape=out,
        grid=(owners // take,),
        in_specs=[*[cut(g.shape) for g in gathered], *[whole] * (len(changes) + 2)],
        out_specs=cut(out.shape),
        scratch_shapes=[
            pltpu.VMEM((take * steps, blocks * depth), jnp.bfloat16),
            pltpu.VMEM((blocks, width, take * steps), jnp.float32),
        ],
        compiler_params=limit(16 if not several else 40),
        name="project",
    )(
        *(gathered if several else held(pltpu.VMEM, *gathered)),
        *held(pltpu.VMEM, *changes, own, other),
    )


def norm_kernel(partial_ref, gain_ref, out_ref, sums_ref, *, groups):
    owners, _, columns = partial_ref.shape
    count = out_ref.shape[0]
    chips = owners // groups // count
    for r in range(count):
        for d in range(groups):
            value = partial_ref[d * chips * count + r]
            for z in range(1, chips):
                value += partial_ref[(d * chips + z) * count + r]
            sums_ref[:, d * columns : (d + 1) * columns] = value
        projected = sums_ref[...]
        mean_square = jnp.mean(projected * projected, axis=1, keepdims=True)
        out_ref[r] = (projected * lax.rsqrt(mean_square + 1e-06) * gain_ref[...]).astype(jnp.bfloat16)


def normalise(partial, gain, groups, count):
    steps, columns = partial.shape[1], partial.shape[2] * groups
    return pl.pallas_call(
        functools.partial(norm_kernel, groups=groups),
        out_shape=jax.ShapeDtypeStruct((count, steps, columns), jnp.bfloat16),
        in_specs=[pl.BlockSpec(memory_space=pltpu.VMEM)] * 2,
        out_specs=pl.BlockSpec(memory_space=pltpu.VMEM),
        scratch_shapes=[pltpu.VMEM((steps, columns), jnp.float32)],
        compiler_params=limit(8),
        name="normalise",
    )(partial, gain.reshape(1, columns))


def body(
    new_weight,
    synced_weight,
    resident,
    gain,
    query,
    cache_keys,
    cache_values,
    new_keys,
    new_values,
    cache_lengths,
):
    groups, devices = lax.axis_size("dp"), lax.axis_size("tensor")
    chips = devices // CORES
    count, steps, _ = query.shape

    def exchange(value, axis, size, unit, hop):
        return lax.ppermute(value, axis, [(i, (i // unit ^ hop) * unit + i % unit) for i in range(size)])

    def fits(size):
        return size <= FEW and size & (size - 1) == 0

    stored = resident.reshape(groups * devices, -1, resident.shape[1])
    attended, own_rows = attend(query, cache_keys, cache_values, new_keys, new_values, cache_lengths, stored, devices)
    other_rows = exchange(own_rows, "tensor", devices, 1, 1)
    near = fits(chips) and fits(groups)
    if near:
        column = [attended]
        for hop in range(1, chips):
            column.append(exchange(attended, "tensor", devices, CORES, hop))
        column = join(column)
    else:
        alike = [[i * CORES + c for i in range(chips)] for c in range(CORES)]
        column = lax.all_gather(attended, "tensor", axis=0, tiled=True, axis_index_groups=alike)
    if near:
        gathered = [column]
        for hop in range(1, groups):
            gathered.append(exchange(column, "dp", groups, 1, hop))
    else:
        gathered = [lax.all_gather(column, "dp", axis=0, tiled=True)]
    own = local_change(new_weight, synced_weight, devices)
    swapped = exchange(own, "tensor", devices, 1, 1)
    partial = project(gathered, [own, swapped], own_rows, other_rows, groups * chips * count, steps)
    summed = lax.all_to_all(
        partial,
        ("dp", "tensor"),
        split_axis=0,
        concat_axis=0,
        tiled=True,
        axis_index_groups=[
            [g * devices + i * CORES + c for g in range(groups) for i in range(chips)] for c in range(CORES)
        ],
    )
    return normalise(summed, gain, groups, count)


def solution(mesh):
    in_specs = (
        P(("dp", "tensor"), None),
        P(("dp", "tensor"), None),
        P(None, "tensor"),
        P(),
        P(("dp", "tensor"), None, None),
        P(("dp", "tensor"), None, None),
        P(("dp", "tensor"), None, None),
        P(("dp", "tensor"), None, None),
        P(("dp", "tensor"), None, None),
        P(("dp", "tensor")),
    )
    out_specs = P(("dp", "tensor"), None, None)
    return jax.shard_map(body, mesh=mesh, in_specs=in_specs, out_specs=out_specs, check_vma=False)
```

```python
import functools

import jax
import jax.numpy as jnp
from jax import lax
from jax.experimental import pallas as pl
from jax.experimental.pallas import tpu as pltpu
from jax.sharding import PartitionSpec as P


HD = 128
CORES = 2
MOST = 32
FEW = 4
NT = (((1,), (1,)), ((), ()))
NN = (((1,), (0,)), ((), ()))


def dot(a, b, dims):
    return lax.dot_general(a, b, dims, preferred_element_type=jnp.float32)


def limit(mebibytes):
    return pltpu.CompilerParams(vmem_limit_bytes=mebibytes << 20)


def held(space, *arrays):
    return [pltpu.with_memory_space_constraint(a, space) for a in arrays]


def divisor(total, most, unit):
    fits = [n for n in range(unit, min(total, most) + 1, unit) if total % n == 0]
    return fits[-1] if fits else total


def attend_kernel(
    lengths_ref,
    query_hbm,
    keys_hbm,
    values_hbm,
    new_keys_hbm,
    new_values_hbm,
    resident_hbm,
    out_ref,
    near_ref,
    query_ref,
    keys_ref,
    values_ref,
    new_keys_ref,
    new_values_ref,
    past_ref,
    own_ref,
    sems,
    *,
    width,
):
    count, steps, features = query_hbm.shape
    _, kv_features = keys_ref.shape
    grouping = features // kv_features
    heads = width // HD
    bands = kv_features // width
    block_rows = grouping * steps
    rows = heads * block_rows
    factor = HD ** (-0.5)
    blocks = near_ref.shape[0]
    near = pltpu.make_async_copy(resident_hbm.at[pl.ds(lax.axis_index("dp") * blocks, blocks)], near_ref, sems.at[5])
    for row in range(count):
        pairs = [
            (query_hbm, query_ref),
            (new_keys_hbm, new_keys_ref),
            (keys_hbm, keys_ref),
            (new_values_hbm, new_values_ref),
            (values_hbm, values_ref),
        ]
        loads = [pltpu.make_async_copy(p[0].at[row], p[1], sems.at[i]) for i, p in enumerate(pairs)]
        for load in loads:
            load.start()
        if row == 0:
            near.start(priority=1)

        padding = jnp.zeros((8 - steps % 8, kv_features), jnp.float32)
        loads[0].wait()
        query = query_ref[...].astype(jnp.float32)
        stacks = []
        for band in range(bands):
            lines = []
            for k in range(heads):
                first = (band * heads + k) * grouping
                pieces = [query[:, (first + g) * HD : (first + g + 1) * HD] for g in range(grouping)]
                own = jnp.concatenate(pieces, axis=0)
                lines.append(jnp.concatenate([own if i == k else jnp.zeros_like(own) for i in range(heads)], axis=1))
            stacks.append(jnp.concatenate(lines, axis=0).astype(jnp.bfloat16))
        loads[1].wait()
        keys_new = jnp.concatenate([new_keys_ref[...].astype(jnp.float32), padding], axis=0).astype(jnp.bfloat16)
        for band in range(bands):
            at = slice(band * width, (band + 1) * width)
            own_ref[band * rows : (band + 1) * rows] = dot(stacks[band], keys_new[:, at], NT)
        loads[2].wait()
        for band in range(bands):
            at = slice(band * width, (band + 1) * width)
            past_ref[band * rows : (band + 1) * rows] = dot(stacks[band], keys_ref[:, at], NT)

        past = past_ref[...] * factor
        own = own_ref[...] * factor
        slot = lax.broadcasted_iota(jnp.int32, past.shape, 1)
        past = jnp.where(slot < lengths_ref[row], past, -jnp.inf)
        column = lax.broadcasted_iota(jnp.int32, own.shape, 1)
        position = lax.rem(lax.broadcasted_iota(jnp.int32, own.shape, 0), steps)
        own = jnp.where(column <= position, own, -jnp.inf)
        highest = jnp.maximum(jnp.max(past, axis=1, keepdims=True), jnp.max(own, axis=1, keepdims=True))
        past = jnp.exp(past - highest)
        own = jnp.exp(own - highest)
        scale = 1.0 / (jnp.sum(past, axis=1, keepdims=True) + jnp.sum(own, axis=1, keepdims=True))
        past = (past * scale).astype(jnp.bfloat16)
        own = (own * scale).astype(jnp.bfloat16)

        loads[3].wait()
        values_new = jnp.concatenate([new_values_ref[...].astype(jnp.float32), padding], axis=0).astype(jnp.bfloat16)
        loads[4].wait()
        for band in range(bands):
            at = slice(band * width, (band + 1) * width)
            lines = slice(band * rows, (band + 1) * rows)
            attended = dot(past[lines], values_ref[:, at], NN) + dot(own[lines], values_new[:, at], NN)
            for k in range(heads):
                for g in range(grouping):
                    head = (band * heads + k) * grouping + g
                    piece = k * block_rows + g * steps
                    value = attended[piece : piece + steps, k * HD : (k + 1) * HD]
                    out_ref[row, :, head * HD : (head + 1) * HD] = value.astype(jnp.bfloat16)
    near.wait()


def attend(query, cache_keys, cache_values, new_keys, new_values, cache_lengths, stored, blocks):
    _, steps, features = query.shape
    slots, kv_features = cache_keys.shape[1:]
    width = HD * 2 if kv_features % (HD * 2) == 0 else HD
    lines = features // HD * steps
    hbm = pl.BlockSpec(memory_space=pltpu.HBM)
    operands = held(pltpu.HBM, query, cache_keys, cache_values, new_keys, new_values)
    return pl.pallas_call(
        functools.partial(attend_kernel, width=width),
        out_shape=[pltpu.VMEM(query.shape, query.dtype), pltpu.VMEM((blocks, *stored.shape[1:]), stored.dtype)],
        in_specs=[pl.BlockSpec(memory_space=pltpu.SMEM), *[hbm] * (len(operands) + 1)],
        out_specs=[pl.BlockSpec(memory_space=pltpu.VMEM)] * 2,
        scratch_shapes=[
            *[pltpu.VMEM(o.shape[1:], o.dtype) for o in operands],
            pltpu.VMEM((lines, slots), jnp.float32),
            pltpu.VMEM((lines, 8 * (steps // 8 + 1)), jnp.float32),
            pltpu.SemaphoreType.DMA((6,)),
        ],
        compiler_params=limit(16),
        name="attend",
    )(cache_lengths, *operands, *held(pltpu.HBM, stored))


def join_kernel(*refs):
    *part_refs, out_ref = refs
    rows = [ref[k].astype(jnp.float32) for ref in part_refs for k in range(ref.shape[0])]
    out_ref[...] = jnp.concatenate(rows, axis=0).astype(out_ref.dtype)


def join(parts):
    whole = pl.BlockSpec(memory_space=pltpu.VMEM)
    count, steps, features = parts[0].shape
    return pl.pallas_call(
        join_kernel,
        out_shape=pltpu.VMEM((len(parts) * count * steps, features), parts[0].dtype),
        in_specs=[whole] * len(parts),
        out_specs=whole,
        compiler_params=limit(4),
        name="join",
    )(*held(pltpu.VMEM, *parts))


def change_kernel(new_ref, synced_ref, out_ref):
    blocks, _, depth = out_ref.shape
    for b in range(blocks):
        columns = slice(b * depth, (b + 1) * depth)
        out_ref[b] = (new_ref[:, columns] - synced_ref[:, columns]).astype(jnp.bfloat16)


def local_change(new_weight, synced_weight, blocks):
    rows, features = new_weight.shape
    whole = pl.BlockSpec(memory_space=pltpu.VMEM)
    return pl.pallas_call(
        change_kernel,
        out_shape=pltpu.VMEM((blocks, rows, features // blocks), jnp.bfloat16),
        in_specs=[whole] * 2,
        out_specs=whole,
        compiler_params=limit(4),
        name="local_change",
    )(*held(pltpu.VMEM, new_weight, synced_weight))


def project_kernel(*refs, parts, cuts):
    gathered, refs = refs[:parts], refs[parts:]
    changes, (own_ref, other_ref, out_ref, rows_ref, sums_ref) = refs[: 2 * cuts], refs[2 * cuts :]
    owners, steps, _ = out_ref.shape
    blocks, _, depth = own_ref.shape
    device = lax.axis_index("tensor")
    places = (device, device ^ 1)
    group, chip = lax.axis_index("dp"), device // CORES

    for i, part in enumerate(gathered):
        if parts > 1:
            value = part[...]
        else:
            pieces = [part[k].astype(jnp.float32) for k in range(owners)]
            value = jnp.concatenate(pieces, axis=0).astype(jnp.bfloat16)
        rows_ref[i * len(value) : (i + 1) * len(value)] = value

    deltas = []
    for ref in changes:
        value = dot(ref[0], rows_ref[:, :depth], NT)
        for b in range(1, blocks):
            value += dot(ref[b], rows_ref[:, b * depth : (b + 1) * depth], NT)
        deltas.append(value)
    for source, ref in enumerate((own_ref, other_ref)):
        rows = rows_ref[:, pl.ds(pl.multiple_of(places[source] * depth, depth), depth)]
        for b in range(blocks):
            value = dot(ref[b], rows, NT)
            if source == 0:
                sums_ref[b] = value
            else:
                sums_ref[b] += value
    for source in range(2):
        first = 0
        for value in deltas[source * cuts : (source + 1) * cuts]:
            sums_ref[places[source], first : first + value.shape[0]] += value
            first += value.shape[0]
    sums = jnp.concatenate([sums_ref[b] for b in range(blocks)], axis=0).T
    each = owners // parts
    for k in range(owners):
        owner = k
        if parts > 1:
            chips = device_count() // CORES
            count = each // chips
            hop, r = k % each // count, k % count
            owner = ((group ^ (k // each)) * chips + (chip ^ hop)) * count + r
        out_ref[owner] = sums[k * steps : (k + 1) * steps]


def device_count():
    return lax.axis_size("tensor")


def project(gathered, changes, own, other, owners, steps):
    blocks, width, depth = own.shape
    take = owners if len(gathered) > 1 else divisor(owners, MOST, 1)
    several = owners > take
    whole = pl.BlockSpec(memory_space=pltpu.VMEM)
    cut = lambda s: pl.BlockSpec((take, *s[1:]), lambda i: (i, 0, 0)) if several else whole
    out = jax.ShapeDtypeStruct((owners, steps, blocks * width), jnp.float32)
    return pl.pallas_call(
        functools.partial(project_kernel, parts=len(gathered), cuts=len(changes) // 2),
        out_shape=out,
        grid=(owners // take,),
        in_specs=[*[cut(g.shape) for g in gathered], *[whole] * (len(changes) + 2)],
        out_specs=cut(out.shape),
        scratch_shapes=[
            pltpu.VMEM((take * steps, blocks * depth), jnp.bfloat16),
            pltpu.VMEM((blocks, width, take * steps), jnp.float32),
        ],
        compiler_params=limit(16 if not several else 40),
        name="project",
    )(
        *(gathered if several else held(pltpu.VMEM, *gathered)),
        *held(pltpu.VMEM, *changes, own, other),
    )


def norm_kernel(partial_ref, gain_ref, out_ref, sums_ref, *, groups):
    owners, _, columns = partial_ref.shape
    count = out_ref.shape[0]
    chips = owners // groups // count
    for r in range(count):
        for d in range(groups):
            value = partial_ref[d * chips * count + r]
            for z in range(1, chips):
                value += partial_ref[(d * chips + z) * count + r]
            sums_ref[:, d * columns : (d + 1) * columns] = value
        projected = sums_ref[...]
        mean_square = jnp.mean(projected * projected, axis=1, keepdims=True)
        out_ref[r] = (projected * lax.rsqrt(mean_square + 1e-06) * gain_ref[...]).astype(jnp.bfloat16)


def normalise(partial, gain, groups, count):
    steps, columns = partial.shape[1], partial.shape[2] * groups
    return pl.pallas_call(
        functools.partial(norm_kernel, groups=groups),
        out_shape=jax.ShapeDtypeStruct((count, steps, columns), jnp.bfloat16),
        in_specs=[pl.BlockSpec(memory_space=pltpu.VMEM)] * 2,
        out_specs=pl.BlockSpec(memory_space=pltpu.VMEM),
        scratch_shapes=[pltpu.VMEM((steps, columns), jnp.float32)],
        compiler_params=limit(8),
        name="normalise",
    )(partial, gain.reshape(1, columns))


def body(
    new_weight,
    synced_weight,
    resident,
    gain,
    query,
    cache_keys,
    cache_values,
    new_keys,
    new_values,
    cache_lengths,
):
    groups, devices = lax.axis_size("dp"), lax.axis_size("tensor")
    chips = devices // CORES
    count, steps, _ = query.shape

    def exchange(value, axis, size, unit, hop):
        return lax.ppermute(value, axis, [(i, (i // unit ^ hop) * unit + i % unit) for i in range(size)])

    def fits(size):
        return size <= FEW and size & (size - 1) == 0

    stored = resident.reshape(groups * devices, -1, resident.shape[1])
    attended, own_rows = attend(query, cache_keys, cache_values, new_keys, new_values, cache_lengths, stored, devices)
    other_rows = exchange(own_rows, "tensor", devices, 1, 1)
    near = fits(chips) and fits(groups)
    if near:
        column = [attended]
        for hop in range(1, chips):
            column.append(exchange(attended, "tensor", devices, CORES, hop))
        column = join(column)
    else:
        alike = [[i * CORES + c for i in range(chips)] for c in range(CORES)]
        column = lax.all_gather(attended, "tensor", axis=0, tiled=True, axis_index_groups=alike)
    if near:
        gathered = [column]
        for hop in range(1, groups):
            gathered.append(exchange(column, "dp", groups, 1, hop))
    else:
        gathered = [lax.all_gather(column, "dp", axis=0, tiled=True)]
    own = local_change(new_weight, synced_weight, devices)
    swapped = exchange(own, "tensor", devices, 1, 1)
    partial = project(gathered, [own, swapped], own_rows, other_rows, groups * chips * count, steps)
    summed = lax.all_to_all(
        partial,
        ("dp", "tensor"),
        split_axis=0,
        concat_axis=0,
        tiled=True,
        axis_index_groups=[
            [g * devices + i * CORES + c for g in range(groups) for i in range(chips)] for c in range(CORES)
        ],
    )
    return normalise(summed, gain, groups, count)


def solution(mesh):
    in_specs = (
        P(("dp", "tensor"), None),
        P(("dp", "tensor"), None),
        P(None, "tensor"),
        P(),
        P(("dp", "tensor"), None, None),
        P(("dp", "tensor"), None, None),
        P(("dp", "tensor"), None, None),
        P(("dp", "tensor"), None, None),
        P(("dp", "tensor"), None, None),
        P(("dp", "tensor")),
    )
    out_specs = P(("dp", "tensor"), None, None)
    return jax.shard_map(body, mesh=mesh, in_specs=in_specs, out_specs=out_specs, check_vma=False)
```
